32 devices in a mesh: blk: 16 (over z, x, core), ang: 2 (over y).
Axes of the slice: x: 2, y: 2, z: 4, core: 2. Of those that a mesh axis runs over, the one named last changes fastest.
Arguments:
- coeffs: bfloat16 [4096, 2048], P('blk'), may hold values from -6 to 6
- orders: int32 [1024], replicated, may hold values from 0 to 47
- plan: int32 [2], replicated, may hold values from 1 to 15
Outputs:
- scores: float32 [2, 4096, 256], P(None, ('blk', 'ang'))
The draws below stay inside these ranges and needn't reach their ends.
Inputs may be any that keep to these rules, and one draw needn't show every extreme that they name: In round r, block b is paired with block b XOR plan[r].
All inputs are finite; a program needn't handle non-finite values.
Results may differ from the reference program's by a relative error of at most 0.002.
Values may be sent and summed in bfloat16 or wider, within the bound.
A program may use at most 64 MiB of HBM per device.

```python
import math
import jax
import jax.numpy as jnp
from jax import lax

IMG_DEV = 256
COEF = 2048
ANGLES = 128
ORDERS = 48
ROUNDS = 2
HALF = 1024
IMAGES = 4096
N_BLK = 16


def with_ends(entries, stream_key, least, high):
    longest = entries.shape.index(max(entries.shape))
    spots = []
    for shift in (0, 1):
        where = [jax.random.randint(jax.random.fold_in(stream_key, axis), (), 0, length) for axis, length in enumerate(entries.shape)]
        where[longest] = (where[longest] + shift) % entries.shape[longest]
        spots.append(tuple(where))
    return entries.at[spots[0]].set(least).at[spots[1]].set(high)


def shard_levels(key, extent, pieces, smallest, largest):
    level, own = 1.0, jax.random.fold_in(key, 6)
    for axis_at, parts in pieces:
        draws = jnp.exp(jax.random.uniform(jax.random.fold_in(own, axis_at), (parts,), jnp.float32, smallest / len(pieces), largest / len(pieces)))
        level = level * jnp.repeat(draws, extent[axis_at] // parts).reshape([-1 if axis == axis_at else 1 for axis in range(len(extent))])
    return level


def normal_values(rng, extent, deviation, reach, pieces=(), kind=jnp.bfloat16):
    loudness = shard_levels(rng, extent, pieces, -0.22, 0.18) if pieces else 1.0
    array = jax.random.normal(rng, extent, jnp.float32) * deviation * loudness
    return jnp.minimum(jnp.maximum(array, -reach), reach).astype(kind)


def setup_inputs(seed: int = 0) -> dict:
    key_of = jax.random.split(jax.random.key(seed), 4)
    return {
        "coeffs": normal_values(key_of[0], (IMAGES, COEF), 1.0, 6.0, ((0, 16),)),
        "orders": with_ends(jax.random.randint(key_of[1], (HALF,), 0, ORDERS), jax.random.fold_in(key_of[1], 1), 0, ORDERS - 1).astype(jnp.int32),
        "plan": jax.random.randint(key_of[2], (ROUNDS,), 1, N_BLK).astype(jnp.int32),
    }


def rotate_rows(block, orders, first_angle, angle_count):
    half_width = block.shape[1] // 2
    real_part = block[:, :half_width].astype(jnp.float32)
    imag_part = block[:, half_width:].astype(jnp.float32)
    angles = (jnp.arange(angle_count) + first_angle).astype(jnp.float32) * (2.0 * math.pi / ANGLES)
    phases = angles[:, None] * orders.astype(jnp.float32)[None, :]
    cosine_table = jnp.cos(phases)[:, None, :]
    sine_table = jnp.sin(phases)[:, None, :]
    rot_real = real_part[None] * cosine_table - imag_part[None] * sine_table
    rot_imag = real_part[None] * sine_table + imag_part[None] * cosine_table
    return jnp.concatenate([rot_real, rot_imag], axis=2).astype(jnp.bfloat16)

def block_best(own_block, partner, orders):
    group_size = 8
    row_count = own_block.shape[0]
    partner_wide = partner.astype(jnp.float32)

    def step(running, step_index):
        rotated = rotate_rows(own_block, orders, step_index * group_size, group_size).astype(jnp.float32)
        stacked = rotated.reshape(group_size * row_count, -1)
        scores_raw = jnp.dot(stacked, partner_wide.T, precision=lax.Precision.HIGHEST, preferred_element_type=jnp.float32)
        return (jnp.maximum(running, scores_raw.reshape(group_size, row_count, -1).max(0)), None)
    start = jnp.full((row_count, partner.shape[0]), -jnp.inf, jnp.float32)
    running, _ = lax.scan(step, start, jnp.arange(ANGLES // group_size, dtype=jnp.int32))
    return running

def reference(coeffs, orders, plan):
    blocks = coeffs.reshape(N_BLK, IMG_DEV, COEF)
    scales = jnp.sqrt(lax.optimization_barrier(jnp.mean(jnp.square(coeffs.astype(jnp.float32)), axis=1)) + 1e-06).reshape(N_BLK, IMG_DEV)
    block_ids = jnp.arange(N_BLK, dtype=jnp.int32)
    round_scores = []
    for round_index in range(ROUNDS):
        partner_ids = jnp.bitwise_xor(block_ids, plan[round_index])

        def per_block(block_index):
            mate = partner_ids[block_index]
            running = block_best(blocks[block_index], blocks[mate], orders)
            return running / (math.sqrt(COEF) * scales[block_index][:, None] * scales[mate][None, :])
        round_scores.append(lax.map(per_block, block_ids).reshape(IMAGES, IMG_DEV))
    return jnp.stack(round_scores)
```

```python
import functools
import math

import jax
import jax.numpy as jnp
import numpy as np
from jax import lax
from jax.experimental import pallas as pl
from jax.experimental.pallas import tpu as pltpu
from jax.sharding import PartitionSpec as P

ANGLES = 128
ORDERS = 48
ROUNDS = 2
LANES = 128
PITCH = 97
ORDER_STEP = 16
IMAGE_STEP = 64
MOST_ROUTES = 128
NT = (((1,), (1,)), ((), ()))


def low_bit(value):
    return value & -value


def side_mask(p, q):
    both = p & q
    plain = jnp.where(both != 0, low_bit(both), low_bit(p) | low_bit(q))
    odd, even = jnp.where(p & 1, p, q), jnp.where(p & 1, q, p)
    rest = even & ~odd
    mixed = jnp.where(rest != 0, 1 | low_bit(rest), plain)
    return jnp.where(both & 1, 1, jnp.where((p | q) & 1, mixed, plain | 1))


def parity(value, bits):
    return sum((value >> bit) & 1 for bit in range(bits)) & 1


def side_mask_of(p, q):
    low = lambda v: v & -v
    both = p & q
    plain = low(both) if both else low(p) | low(q)
    if both & 1:
        return 1
    if (p | q) & 1:
        odd, even = (p, q) if p & 1 else (q, p)
        rest = even & ~odd
        return 1 | low(rest) if rest else plain
    return plain | 1


def routes(n_blk):
    there, back = [], []
    for p in range(1, n_blk):
        for q in range(p, n_blk):
            mask = side_mask_of(p, q)
            assert bin(mask & p).count("1") % 2 and bin(mask & q).count("1") % 2
            pairs = [(b, b ^ (q if bin(mask & b).count("1") % 2 else p)) for b in range(n_blk)]
            assert sorted(t for _, t in pairs) == list(range(n_blk))
            there.append(pairs)
            back.append([(t, s) for s, t in pairs])
    return there, back


def angle_table():
    theta = 2.0 * math.pi * np.arange(ANGLES) / ANGLES
    phase = theta[:, None] * np.arange(ORDERS)[None, :]
    full = np.concatenate([np.cos(phase), np.sin(phase)], axis=1)
    high = full.astype(np.float32).astype(jnp.bfloat16)
    low = (full - high.astype(np.float64)).astype(np.float32).astype(jnp.bfloat16)
    return np.concatenate([high, low], axis=1)


def sort_kernel(plan_ref, orders_ref, x_hbm, own_ref, send_ref, route_ref, perm, x_ref, arrived):
    fetch = pltpu.make_async_copy(x_hbm, x_ref, arrived)
    fetch.start()
    blk_count = lax.axis_size("blk")
    low, high = jnp.minimum(plan_ref[0], plan_ref[1]), jnp.maximum(plan_ref[0], plan_ref[1])
    side = parity(side_mask(low, high) & lax.axis_index("blk"), blk_count.bit_length() - 1)
    route_ref[0] = (low - 1) * blk_count - (((low - 1) * low) >> 1) + high - low
    route_ref[1] = side
    route_ref[2] = (1 - side) ^ jnp.where(plan_ref[0] > plan_ref[1], 1, 0)
    half = orders_ref.shape[1]
    chunks = half // LANES
    slot = lax.broadcasted_iota(jnp.int32, (1, half), 1)
    key = (orders_ref[...] * half + slot).astype(jnp.float32)
    lane = lax.broadcasted_iota(jnp.int32, (LANES, half), 1).astype(jnp.float32)
    for c in range(chunks):
        piece = key[:, c * LANES : (c + 1) * LANES]
        column = jnp.broadcast_to(piece, (LANES, LANES)).T
        count = jnp.zeros((LANES, LANES), jnp.float32)
        for d in range(chunks):
            other = key[:, d * LANES : (d + 1) * LANES]
            count += jnp.where(other < column, 1.0, 0.0)
        rank = jnp.sum(count, axis=1, keepdims=True)
        perm[c * LANES : (c + 1) * LANES, :] = jnp.where(lane == rank, 1.0, 0.0).astype(jnp.bfloat16)
    fetch.wait()
    width = 2 * LANES
    for d in range(half // width):
        p = perm[:, d * width : (d + 1) * width]
        for part in range(2):
            got = jnp.dot(
                x_ref[:, part * half : (part + 1) * half], p, preferred_element_type=jnp.float32
            ).astype(jnp.bfloat16)
            for e in range(2):
                at = ((2 * d + e) * 2 + part) * LANES
                own_ref[:, at : at + LANES] = got[:, e * LANES : (e + 1) * LANES]
    share = send_ref.shape[1]
    first = pl.multiple_of(lax.axis_index("ang") * share, share)
    for at in range(0, 2 * half, LANES):
        send_ref[at : at + LANES, :] = own_ref[pl.ds(first, share), at : at + LANES].T


def pair_kernel(starts, heads, own_ref, mate_ref, table_ref, mine_ref, other_ref, turned_ref, grid, best):
    rows, cols = own_ref.shape
    mates = mate_ref.shape[1]
    width = 2 * LANES
    slots = lax.broadcasted_iota(jnp.int32, (LANES, mates), 0)

    def product(chunk, low, high):
        at = chunk * width if isinstance(chunk, int) else pl.multiple_of(chunk * width, width)
        place = slots + chunk * LANES
        keep = jnp.where((place >= low) & (place < high), 1.0, 0.0).astype(jnp.bfloat16)
        u = mate_ref[pl.ds(at, LANES), :] * keep
        v = mate_ref[pl.ds(at + LANES, LANES), :] * keep
        w = jnp.concatenate(
            [jnp.concatenate([u, v], axis=1), jnp.concatenate([v, -u], axis=1)], axis=0
        )
        return jnp.dot(own_ref[:, pl.ds(at, width)], w, preferred_element_type=jnp.float32)

    def spread(k, value):
        for i in range(0, rows, 8):
            grid[pl.ds(i * PITCH + k, 8, stride=PITCH), :] = value[i : i + 8, :mates]
            grid[pl.ds(i * PITCH + k + ORDERS, 8, stride=PITCH), :] = value[i : i + 8, mates:]

    def first_chunks(step, carry):
        for e in range(ORDER_STEP):
            k = step * ORDER_STEP + e
            low = starts[k]
            spread(k, product(jnp.minimum(low // LANES, cols // width - 1), low, starts[k + 1]))
        return carry

    lax.fori_loop(0, ORDERS // ORDER_STEP, first_chunks, 0)

    for chunk in range(1, cols // width):
        k = heads[chunk]
        low = jnp.where(starts[k] < chunk * LANES, starts[k], starts[k + 1])
        value = product(chunk, low, starts[k + 1])
        for i in range(0, rows, 8):
            cos_at = pl.ds(i * PITCH + k, 8, stride=PITCH)
            sin_at = pl.ds(i * PITCH + k + ORDERS, 8, stride=PITCH)
            grid[cos_at, :] += value[i : i + 8, :mates]
            grid[sin_at, :] += value[i : i + 8, mates:]

    table = table_ref[...]

    def image_step(step, carry):
        base = pl.multiple_of(step * IMAGE_STEP, IMAGE_STEP)
        rows_out = []
        for i in range(0, IMAGE_STEP, 2):
            pieces = []
            for e in range(2):
                at = (base + i + e) * PITCH
                pieces.append(grid[pl.ds(at, 2 * ORDERS), :].astype(jnp.bfloat16))
            d = jnp.concatenate(pieces, axis=1)
            d = jnp.concatenate([d, d], axis=0)
            raw = jnp.dot(table, d, preferred_element_type=jnp.float32)
            top = jnp.max(raw, axis=0, keepdims=True)
            rows_out += [top[:, :mates], top[:, mates:]]
        best[pl.ds(base, IMAGE_STEP), :] = jnp.concatenate(rows_out, axis=0)
        return carry

    lax.fori_loop(0, rows // IMAGE_STEP, image_step, 0)

    def rms(ref, axis):
        x = ref[...].astype(jnp.float32)
        return jnp.sqrt(jnp.sum(x * x, axis=axis, keepdims=True) * (1.0 / cols) + 1e-06)

    scores = best[...] / (math.sqrt(cols) * rms(own_ref, 1) * rms(mate_ref, 0))
    best[...] = scores
    turned_ref[...] = scores.T
    share = mine_ref.shape[0]
    ang = lax.axis_index("ang")
    mine_ref[...] = best[pl.ds(pl.multiple_of(ang * share, share), share), :]
    if other_ref.shape[0] * 2 == rows:
        other_ref[...] = best[pl.ds(pl.multiple_of((1 - ang) * share, share), share), :]
    else:
        other_ref[...] = jnp.zeros_like(other_ref)


def per_device_wide(tables, coeffs, orders, plan):
    there, back = tables
    ang_count = lax.axis_size("ang")
    ang_index = lax.axis_index("ang")
    rows, cols = coeffs.shape
    share = rows // ang_count
    half = cols // 2
    blk_count = lax.axis_size("blk")
    low, high = jnp.minimum(plan[0], plan[1]), jnp.maximum(plan[0], plan[1])
    starts = jnp.sum(orders[None, :] < jnp.arange(ORDERS + 1)[:, None], axis=1).astype(jnp.int32)
    firsts = jnp.arange(half // LANES) * LANES
    heads = jnp.sum(starts[1:, None] <= firsts[None, :], axis=0).astype(jnp.int32)

    vmem = pl.BlockSpec(memory_space=pltpu.VMEM)
    smem = pl.BlockSpec(memory_space=pltpu.SMEM)
    params = pltpu.CompilerParams(vmem_limit_bytes=48 * 1024 * 1024)
    own, send, chosen = pl.pallas_call(
        sort_kernel,
        out_shape=(
            jax.ShapeDtypeStruct((rows, cols), jnp.bfloat16),
            jax.ShapeDtypeStruct((cols, share), jnp.bfloat16),
            jax.ShapeDtypeStruct((3,), jnp.int32),
        ),
        in_specs=[smem, vmem, pl.BlockSpec(memory_space=pltpu.HBM)],
        out_specs=(vmem, vmem, smem),
        scratch_shapes=[
            pltpu.VMEM((half, half), jnp.bfloat16),
            pltpu.VMEM((rows, cols), jnp.bfloat16),
            pltpu.SemaphoreType.DMA,
        ],
        compiler_params=params,
    )(plan, orders[None, :], coeffs)
    route, side, active = chosen[0], chosen[1], chosen[2]

    def over(value, choices, side_of_low):
        if len(choices) <= MOST_ROUTES:
            branches = [
                functools.partial(lambda pairs, v: lax.ppermute(v, "blk", pairs), pairs) for pairs in choices
            ]
            return lax.switch(route, branches, value)
        got = []
        for offset in (low, high):
            held = value
            for bit in range(blk_count.bit_length() - 1):
                pairs = [(b, b ^ (1 << bit)) for b in range(blk_count)]
                wanted = ((offset >> bit) & 1) == 1
                held = jnp.where(wanted, lax.ppermute(held, "blk", pairs), held)
            got.append(held)
        return jnp.where(side == side_of_low, got[0], got[1])

    mate = over(send, there, 1)
    wide = -(-share // LANES) * LANES
    mate = jnp.pad(mate, ((0, 0), (0, wide - share)))
    block = jax.ShapeDtypeStruct((share, wide), jnp.float32)
    mine, other, turned = pl.pallas_call(
        pair_kernel,
        out_shape=(block, block, jax.ShapeDtypeStruct((wide, rows), jnp.float32)),
        in_specs=[smem, smem, vmem, vmem, vmem],
        out_specs=(vmem, vmem, vmem),
        scratch_shapes=[
            pltpu.VMEM((rows * PITCH, wide), jnp.float32),
            pltpu.VMEM((rows, wide), jnp.float32),
        ],
        compiler_params=params,
    )(starts, heads, own, mate, jnp.asarray(angle_table()))
    sent = over(turned[:share], back, 0)
    if ang_count == 2:
        across = lax.ppermute(other, "ang", [(0, 1), (1, 0)])
        here = jnp.where(
            ang_index == 0,
            jnp.concatenate([mine, across], axis=1),
            jnp.concatenate([across, mine], axis=1),
        )
    else:
        pieces = turned[:share].T.reshape(ang_count, share, share)
        pieces = lax.all_to_all(pieces, "ang", 0, 0)
        here = pieces.transpose(1, 0, 2).reshape(share, rows)
    return jnp.where(
        active == 0, jnp.stack([here, sent]), jnp.stack([sent, here])
    )


MESH = pl.DeviceIdType.MESH
PRODUCTS = 8
IMAGES = 64


def slots_of(half):
    return ORDERS + half // LANES


def flipped(index, bits):
    for bit in range(bits.bit_length()):
        if (bits >> bit) & 1:
            index = index + (1 - 2 * bit_of(index, bit)) * (1 << bit)
    return index


def bit_of(index, bit):
    return lax.rem(lax.div(index, 1 << bit), 2)


def greet(devices):
    barrier = pltpu.get_barrier_semaphore()
    for device in devices:
        pl.semaphore_signal(barrier, inc=1, device_id=device, device_id_type=MESH)
    pl.semaphore_wait(barrier, len(devices))


def remote(source, target, sent, arrived, device):
    return pltpu.make_async_remote_copy(
        src_ref=source,
        dst_ref=target,
        send_sem=sent,
        recv_sem=arrived,
        device_id=device,
        device_id_type=MESH,
    )


def swap_kernel(orders_hbm, table_hbm, plan_hbm, x_hbm, both_ref, perm_hbm, marks_ref, angles_ref, route_0, route_1,
                flips_ref, orders_ref, table_ref, plan_ref, perm_ref, fetched, stored, sent, arrived):
    me = lax.axis_index("blk")
    sibling = {"blk": flipped(me, 1)}
    fetches = [
        pltpu.make_async_copy(source, target, fetched.at[n])
        for n, (source, target) in enumerate(
            [(orders_hbm, orders_ref), (plan_hbm, plan_ref), (table_hbm, table_ref), (x_hbm, both_ref.at[0])]
        )
    ]
    for fetch in fetches:
        fetch.start()
    greet([sibling])
    swap = remote(x_hbm, both_ref.at[1], sent, arrived, sibling)
    swap.start()
    for fetch in fetches:
        fetch.wait()
    route_0[0], route_1[0] = plan_ref[0] >> 1, plan_ref[1] >> 1
    which = lax.broadcasted_iota(jnp.int32, flips_ref.shape, 0)
    even = jnp.where(which == 0, plan_ref[0], plan_ref[1]) & 1
    flips_ref[...] = 1.0 - even.astype(jnp.float32)

    half = orders_ref.shape[1]
    chunks = half // LANES
    slots = slots_of(half)
    orders = orders_ref[...].astype(jnp.float32)
    order = lax.broadcasted_iota(jnp.int32, (ORDERS, half), 0).astype(jnp.float32)
    ends = jnp.sum(jnp.where(orders <= order, 1.0, 0.0), axis=1, keepdims=True)

    def ended_before(place):
        return jnp.sum(jnp.where(ends <= place, 1.0, 0.0), axis=0, keepdims=True)

    def end_of(which):
        shape = (ORDERS, which.shape[1])
        row = lax.broadcasted_iota(jnp.int32, shape, 0).astype(jnp.float32)
        return jnp.sum(jnp.where(row == which, ends, 0.0), axis=0, keepdims=True)

    lane = lax.broadcasted_iota(jnp.int32, (1, LANES), 1).astype(jnp.float32)
    edge = (lane - ORDERS) * LANES
    late = lane >= ORDERS
    owner = jnp.where(late, ended_before(edge), lane)
    start, end = end_of(owner - 1), end_of(owner)
    chunk = jnp.zeros_like(lane)
    for c in range(1, chunks):
        chunk += jnp.where(start >= c * LANES, 1.0, 0.0)
    chunk = jnp.where(late, lane - ORDERS, chunk)
    low = jnp.where(late & (start >= edge), end, start) - chunk * LANES
    marks_ref[...] = jnp.concatenate([chunk, low, end - chunk * LANES], axis=0).astype(jnp.int32)

    wide = angles_ref.shape[1]
    place = lax.broadcasted_iota(jnp.int32, (1, wide), 1)
    part = sum(jnp.where(place >= slots * n, 1, 0) for n in range(1, 4))
    slot = (place - part * slots).astype(jnp.float32)
    wanted = jnp.where(slot < ORDERS, slot, ended_before((slot - ORDERS) * LANES))
    wanted = wanted + part.astype(jnp.float32) * ORDERS
    index = lax.broadcasted_iota(jnp.int32, (table_ref.shape[1], wide), 0).astype(jnp.float32)
    pick = jnp.where(index == wanted, 1.0, 0.0).astype(jnp.bfloat16)
    angles_ref[...] = jnp.dot(
        table_ref[...], pick, preferred_element_type=jnp.float32
    ).astype(jnp.bfloat16)

    spot = lax.broadcasted_iota(jnp.int32, (1, half), 1).astype(jnp.float32)
    key = orders * half + spot
    columns = [
        jnp.broadcast_to(key[:, c * LANES : (c + 1) * LANES], (LANES, LANES)).T for c in range(chunks)
    ]
    sub = lax.broadcasted_iota(jnp.int32, (half, LANES), 0).astype(jnp.float32)
    for d in range(chunks):
        piece = key[:, d * LANES : (d + 1) * LANES]
        count = jnp.zeros((LANES, LANES), jnp.float32)
        for c in range(chunks):
            count += jnp.where(columns[c] < piece, 1.0, 0.0)
        rank = jnp.sum(count, axis=0, keepdims=True)
        perm_ref[:, d * LANES : (d + 1) * LANES] = jnp.where(sub == rank, 1.0, 0.0).astype(jnp.bfloat16)
    store = pltpu.make_async_copy(perm_ref, perm_hbm, stored)
    store.start()
    swap.wait()
    store.wait()


def round_kernel(core, offset, flips_ref, marks_ref, both_ref, perm_hbm, angles_ref, keep_ref, give_ref,
                 perm_ref, fetched, local, offered, raw, own, mate, grid, best, scale, near, far, sent, arrived):
    me = lax.axis_index("blk")
    ang = lax.axis_index("ang")
    rows, cols = both_ref.shape[1:]
    half = cols // 2
    share = raw.shape[0]
    slots = slots_of(half)
    pitch = grid.shape[0] // rows
    width = 2 * LANES
    blocks = rows // IMAGES
    partner = {"blk": flipped(me, 2 * offset)}
    beside = {"ang": 1 - ang}

    def body():
        side = bit_of(me, low_bit(offset).bit_length()) if offset else 0
        swapped = flips_ref[core : core + 1, :1] * lax.convert_element_type(side, jnp.float32)
        flip = swapped.astype(jnp.bfloat16)
        stay = 1 - flip
        first = pl.multiple_of(ang * share, share)
        target = offered if offset else raw
        fetch = pltpu.make_async_copy(perm_hbm, perm_ref, fetched)
        fetch.start()

        def fill(step, carry):
            at = pl.multiple_of(step * 32, 32)
            here = pl.ds(first + at, 32)
            target[pl.ds(at, 32), :] = both_ref[0, here, :] * stay + both_ref[1, here, :] * flip
            return carry

        lax.fori_loop(0, share // 32, fill, 0)
        greet([partner, beside] if offset else [beside])
        if offset:
            offer = remote(offered, raw, sent.at[0], arrived.at[0], partner)
            offer.start()

        def norms(step, carry):
            here = pl.ds(pl.multiple_of(step * 32, 32), 32)
            x = both_ref[1, here, :] * stay + both_ref[0, here, :] * flip
            local[here, :] = x
            x = x.astype(jnp.float32)
            power = jnp.sum(x * x, axis=1, keepdims=True) * (1.0 / cols)
            rms = math.sqrt(cols) * jnp.sqrt(power + 1e-06)
            scale[here, :] = jnp.broadcast_to(1.0 / rms, (32, share))
            return carry

        lax.fori_loop(0, rows // 32, norms, 0)

        def sort_own(step, carry):
            d, part = lax.div(step, 2), lax.rem(step, 2)
            p = perm_ref[pl.ds(pl.multiple_of(d * width, width), width), :]
            x = local[:, pl.ds(pl.multiple_of(part * half, half), half)]
            got = lax.dot_general(x, p, NT, preferred_element_type=jnp.float32).astype(jnp.bfloat16)
            for e in range(2):
                own[2 * d + e, :, pl.ds(pl.multiple_of(part * LANES, LANES), LANES)] = got[
                    :, e * LANES : (e + 1) * LANES
                ]
            return carry

        fetch.wait()
        lax.fori_loop(0, cols // width, sort_own, 0)
        if offset:
            offer.wait()

        pair = jnp.concatenate([raw[:, :half], raw[:, half:]], axis=0)

        def sort_mates(step, carry):
            p = perm_ref[pl.ds(pl.multiple_of(step * 2 * width, 2 * width), 2 * width), :]
            got = lax.dot_general(p, pair, NT, preferred_element_type=jnp.float32)
            for e in range(4):
                mate[step * 4 + e] = got[e * LANES : (e + 1) * LANES].astype(jnp.bfloat16)
            return carry + jnp.sum(got * got, axis=0, keepdims=True)

        power = lax.fori_loop(
            0, half // (2 * width), sort_mates, jnp.zeros((1, 2 * share), jnp.float32)
        )
        power = (power[:, :share] + power[:, share:]) * (1.0 / cols)
        mates = 1.0 / jnp.sqrt(power + 1e-06)
        places = lax.broadcasted_iota(jnp.int32, (LANES, share), 0)

        def product(slot):
            chunk, low, high = marks_ref[0, slot], marks_ref[1, slot], marks_ref[2, slot]
            keep = jnp.where((places >= low) & (places < high), 1.0, 0.0).astype(jnp.bfloat16)
            uv = mate[chunk]
            u, v = uv[:, :share] * keep, uv[:, share:] * keep
            w = jnp.concatenate(
                [jnp.concatenate([u, v], axis=1), jnp.concatenate([v, -u], axis=1)], axis=0
            )
            return jnp.dot(own[chunk], w, preferred_element_type=jnp.float32)

        def products(step, carry):
            for e in range(PRODUCTS):
                slot = step * PRODUCTS + e
                value = product(slot)
                for i in range(0, rows, 8):
                    grid[pl.ds(i * pitch + slot, 8, stride=pitch), :] = value[i : i + 8, :share]
                    grid[pl.ds(i * pitch + slot + slots, 8, stride=pitch), :] = value[i : i + 8, share:]
            return carry

        lax.fori_loop(0, slots // PRODUCTS, products, 0)

        angles = angles_ref[:, : 4 * slots]
        early = blocks // 2

        def base_of(step):
            return pl.multiple_of(lax.rem(step + early * (1 - ang), blocks) * IMAGES, IMAGES)

        def back(step):
            piece = pl.ds(base_of(step), IMAGES)
            return remote(best.at[piece, :], far.at[piece, :], sent.at[1 + step], arrived.at[1 + step], partner)

        def across(step):
            return remote(
                best.at[pl.ds(base_of(step), IMAGES), :],
                near.at[pl.ds(pl.multiple_of(step * IMAGES, IMAGES), IMAGES), :],
                sent.at[1 + blocks + step],
                arrived.at[1 + blocks + step],
                beside,
            )

        def ship(step):
            if offset:
                back(step).start()
            pl.when(step < early)(lambda: across(step).start())

        def images(step, carry):
            base = base_of(step)
            tops = []
            for i in range(0, IMAGES, 2):
                pieces = [
                    grid[pl.ds((base + i + e) * pitch, 2 * slots), :].astype(jnp.bfloat16) for e in range(2)
                ]
                d = jnp.concatenate(pieces, axis=1)
                d = jnp.concatenate([d, d], axis=0)
                score = jnp.dot(angles, d, preferred_element_type=jnp.float32)
                top = jnp.max(score, axis=0, keepdims=True)
                tops += [top[:, :share], top[:, share:]]
            top = jnp.concatenate(tops, axis=0)
            best[pl.ds(base, IMAGES), :] = top * scale[pl.ds(base, IMAGES), :] * mates
            pl.when(step > 0)(lambda: ship(step - 1))
            return carry

        lax.fori_loop(0, blocks, images, 0)
        ship(blocks - 1)
        for step in range(early):
            across(step).wait()
        mine, other = best[pl.ds(first, share), :], near[...]
        ahead = lax.broadcasted_iota(jnp.int32, (share, share), 0) * 0 + ang == 0
        here = jnp.concatenate(
            [jnp.where(ahead, mine, other), jnp.where(ahead, other, mine)], axis=1
        )
        if offset:
            for step in range(blocks):
                back(step).wait()
            there = far[...].T
        else:
            there = best[...].T
        local_own = jnp.broadcast_to(swapped, (share, rows)) > 0.5
        keep_ref[...] = jnp.where(local_own, here, there)
        give_ref[...] = jnp.where(local_own, there, here)

    pl.when(bit_of(me, 0) == core)(body)


def last_kernel(keep_0, give_0, keep_1, give_1, out_ref, sent, arrived):
    me = lax.axis_index("blk")
    sibling = {"blk": flipped(me, 1)}
    greet([sibling])

    def finish(core, keep, give):
        def body():
            copy = remote(give, out_ref.at[core], sent, arrived, sibling)
            copy.start()
            out_ref[core] = keep[...]
            copy.wait_send()
            remote(give, out_ref.at[1 - core], sent, arrived, sibling).wait_recv()

        pl.when(bit_of(me, 0) == core)(body)

    finish(0, keep_0, give_0)
    finish(1, keep_1, give_1)


def per_device(coeffs, orders, plan):
    rows, cols = coeffs.shape
    share = rows // lax.axis_size("ang")
    half = cols // 2
    chips = lax.axis_size("blk") // 2
    slots = slots_of(half)
    wide = -(-4 * slots // LANES) * LANES
    vmem = pl.BlockSpec(memory_space=pltpu.VMEM)
    smem = pl.BlockSpec(memory_space=pltpu.SMEM)
    hbm = pl.BlockSpec(memory_space=pltpu.HBM)

    def params(number, mib):
        return pltpu.CompilerParams(
            has_side_effects=True, collective_id=number, vmem_limit_bytes=mib * 1024 * 1024
        )

    far_off = functools.partial(pltpu.with_memory_space_constraint, memory_space=pltpu.HBM)
    table = angle_table()
    number = jax.ShapeDtypeStruct((1,), jnp.int32)
    both, perm, marks, angles, route_0, route_1, flips = pl.pallas_call(
        swap_kernel,
        out_shape=(
            jax.ShapeDtypeStruct((2, rows, cols), jnp.bfloat16),
            jax.ShapeDtypeStruct((half, half), jnp.bfloat16),
            jax.ShapeDtypeStruct((3, LANES), jnp.int32),
            jax.ShapeDtypeStruct((ANGLES, wide), jnp.bfloat16),
            number,
            number,
            jax.ShapeDtypeStruct((8, LANES), jnp.float32),
        ),
        in_specs=[hbm] * 4,
        out_specs=(vmem, hbm, vmem, vmem, smem, smem, vmem),
        scratch_shapes=[
            pltpu.VMEM((1, half), jnp.int32),
            pltpu.VMEM(table.shape, jnp.bfloat16),
            pltpu.SMEM((ROUNDS,), jnp.int32),
            pltpu.VMEM((half, half), jnp.bfloat16),
            pltpu.SemaphoreType.DMA((4,)),
            pltpu.SemaphoreType.DMA,
            pltpu.SemaphoreType.DMA,
            pltpu.SemaphoreType.DMA,
        ],
        compiler_params=params(0, 6),
    )(*[far_off(value) for value in (orders[None, :], jnp.asarray(table), plan, coeffs)])

    result = jax.ShapeDtypeStruct((share, rows), jnp.float32)
    copies = 1 + rows // IMAGES + share // IMAGES
    found = []
    for core, route in enumerate((route_0, route_1)):
        rounds = [
            pl.pallas_call(
                functools.partial(round_kernel, core, offset),
                out_shape=(result, result),
                in_specs=[vmem, smem, vmem, hbm, vmem],
                out_specs=(vmem, vmem),
                scratch_shapes=[
                    pltpu.VMEM((half, half), jnp.bfloat16),
                    pltpu.SemaphoreType.DMA,
                    pltpu.VMEM((rows, cols), jnp.bfloat16),
                    pltpu.VMEM((share, cols), jnp.bfloat16),
                    pltpu.VMEM((share, cols), jnp.bfloat16),
                    pltpu.VMEM((half // LANES, rows, 2 * LANES), jnp.bfloat16),
                    pltpu.VMEM((half // LANES, LANES, 2 * share), jnp.bfloat16),
                    pltpu.VMEM((rows * (2 * slots + 1), share), jnp.float32),
                    pltpu.VMEM((rows, share), jnp.float32),
                    pltpu.VMEM((rows, share), jnp.float32),
                    pltpu.VMEM((share, share), jnp.float32),
                    pltpu.VMEM((rows, share), jnp.float32),
                    pltpu.SemaphoreType.DMA((copies,)),
                    pltpu.SemaphoreType.DMA((copies,)),
                ],
                compiler_params=params(1 + core * chips + offset, 26),
            )
            for offset in range(chips)
        ]
        found += lax.switch(route[0], rounds, flips, marks, both, perm, angles)
    return pl.pallas_call(
        last_kernel,
        out_shape=jax.ShapeDtypeStruct((ROUNDS, share, rows), jnp.float32),
        in_specs=[vmem] * 4,
        out_specs=vmem,
        scratch_shapes=[pltpu.SemaphoreType.DMA] * 2,
        compiler_params=params(1 + 2 * chips, 8),
    )(*found)


def solution(mesh):
    n_blk, n_ang = mesh.shape["blk"], mesh.shape["ang"]
    body = per_device if n_blk <= 16 and n_ang == 2 else functools.partial(per_device_wide, routes(n_blk))
    return jax.shard_map(
        body,
        mesh=mesh,
        in_specs=(P("blk", None), P(), P()),
        out_specs=P(None, ("blk", "ang"), None),
        check_vma=False,
    )
```

```python
import functools
import math

import jax
import jax.numpy as jnp
import numpy as np
from jax import lax
from jax.experimental import pallas as pl
from jax.experimental.pallas import tpu as pltpu
from jax.sharding import PartitionSpec as P

ANGLES = 128
ORDERS = 48
ROUNDS = 2
LANES = 128
PITCH = 97
ORDER_STEP = 16
IMAGE_STEP = 64
MOST_ROUTES = 128
NT = (((1,), (1,)), ((), ()))


def low_bit(value):
    return value & -value


def side_mask(p, q):
    both = p & q
    plain = jnp.where(both != 0, low_bit(both), low_bit(p) | low_bit(q))
    odd, even = jnp.where(p & 1, p, q), jnp.where(p & 1, q, p)
    rest = even & ~odd
    mixed = jnp.where(rest != 0, 1 | low_bit(rest), plain)
    return jnp.where(both & 1, 1, jnp.where((p | q) & 1, mixed, plain | 1))


def parity(value, bits):
    return sum((value >> bit) & 1 for bit in range(bits)) & 1


def side_mask_of(p, q):
    low = lambda v: v & -v
    both = p & q
    plain = low(both) if both else low(p) | low(q)
    if both & 1:
        return 1
    if (p | q) & 1:
        odd, even = (p, q) if p & 1 else (q, p)
        rest = even & ~odd
        return 1 | low(rest) if rest else plain
    return plain | 1


def routes(n_blk):
    there, back = [], []
    for p in range(1, n_blk):
        for q in range(p, n_blk):
            mask = side_mask_of(p, q)
            assert bin(mask & p).count("1") % 2 and bin(mask & q).count("1") % 2
            pairs = [(b, b ^ (q if bin(mask & b).count("1") % 2 else p)) for b in range(n_blk)]
            assert sorted(t for _, t in pairs) == list(range(n_blk))
            there.append(pairs)
            back.append([(t, s) for s, t in pairs])
    return there, back


def angle_table():
    theta = 2.0 * math.pi * np.arange(ANGLES) / ANGLES
    phase = theta[:, None] * np.arange(ORDERS)[None, :]
    full = np.concatenate([np.cos(phase), np.sin(phase)], axis=1)
    high = full.astype(np.float32).astype(jnp.bfloat16)
    low = (full - high.astype(np.float64)).astype(np.float32).astype(jnp.bfloat16)
    return np.concatenate([high, low], axis=1)


def sort_kernel(plan_ref, orders_ref, x_hbm, own_ref, send_ref, route_ref, perm, x_ref, arrived):
    fetch = pltpu.make_async_copy(x_hbm, x_ref, arrived)
    fetch.start()
    blk_count = lax.axis_size("blk")
    low, high = jnp.minimum(plan_ref[0], plan_ref[1]), jnp.maximum(plan_ref[0], plan_ref[1])
    side = parity(side_mask(low, high) & lax.axis_index("blk"), blk_count.bit_length() - 1)
    route_ref[0] = (low - 1) * blk_count - (((low - 1) * low) >> 1) + high - low
    route_ref[1] = side
    route_ref[2] = (1 - side) ^ jnp.where(plan_ref[0] > plan_ref[1], 1, 0)
    half = orders_ref.shape[1]
    chunks = half // LANES
    slot = lax.broadcasted_iota(jnp.int32, (1, half), 1)
    key = (orders_ref[...] * half + slot).astype(jnp.float32)
    lane = lax.broadcasted_iota(jnp.int32, (LANES, half), 1).astype(jnp.float32)
    for c in range(chunks):
        piece = key[:, c * LANES : (c + 1) * LANES]
        column = jnp.broadcast_to(piece, (LANES, LANES)).T
        count = jnp.zeros((LANES, LANES), jnp.float32)
        for d in range(chunks):
            other = key[:, d * LANES : (d + 1) * LANES]
            count += jnp.where(other < column, 1.0, 0.0)
        rank = jnp.sum(count, axis=1, keepdims=True)
        perm[c * LANES : (c + 1) * LANES, :] = jnp.where(lane == rank, 1.0, 0.0).astype(jnp.bfloat16)
    fetch.wait()
    width = 2 * LANES
    for d in range(half // width):
        p = perm[:, d * width : (d + 1) * width]
        for part in range(2):
            got = jnp.dot(
                x_ref[:, part * half : (part + 1) * half], p, preferred_element_type=jnp.float32
            ).astype(jnp.bfloat16)
            for e in range(2):
                at = ((2 * d + e) * 2 + part) * LANES
                own_ref[:, at : at + LANES] = got[:, e * LANES : (e + 1) * LANES]
    share = send_ref.shape[1]
    first = pl.multiple_of(lax.axis_index("ang") * share, share)
    for at in range(0, 2 * half, LANES):
        send_ref[at : at + LANES, :] = own_ref[pl.ds(first, share), at : at + LANES].T


def pair_kernel(starts, heads, own_ref, mate_ref, table_ref, mine_ref, other_ref, turned_ref, grid, best):
    rows, cols = own_ref.shape
    mates = mate_ref.shape[1]
    width = 2 * LANES
    slots = lax.broadcasted_iota(jnp.int32, (LANES, mates), 0)

    def product(chunk, low, high):
        at = chunk * width if isinstance(chunk, int) else pl.multiple_of(chunk * width, width)
        place = slots + chunk * LANES
        keep = jnp.where((place >= low) & (place < high), 1.0, 0.0).astype(jnp.bfloat16)
        u = mate_ref[pl.ds(at, LANES), :] * keep
        v = mate_ref[pl.ds(at + LANES, LANES), :] * keep
        w = jnp.concatenate(
            [jnp.concatenate([u, v], axis=1), jnp.concatenate([v, -u], axis=1)], axis=0
        )
        return jnp.dot(own_ref[:, pl.ds(at, width)], w, preferred_element_type=jnp.float32)

    def spread(k, value):
        for i in range(0, rows, 8):
            grid[pl.ds(i * PITCH + k, 8, stride=PITCH), :] = value[i : i + 8, :mates]
            grid[pl.ds(i * PITCH + k + ORDERS, 8, stride=PITCH), :] = value[i : i + 8, mates:]

    def first_chunks(step, carry):
        for e in range(ORDER_STEP):
            k = step * ORDER_STEP + e
            low = starts[k]
            spread(k, product(jnp.minimum(low // LANES, cols // width - 1), low, starts[k + 1]))
        return carry

    lax.fori_loop(0, ORDERS // ORDER_STEP, first_chunks, 0)

    for chunk in range(1, cols // width):
        k = heads[chunk]
        low = jnp.where(starts[k] < chunk * LANES, starts[k], starts[k + 1])
        value = product(chunk, low, starts[k + 1])
        for i in range(0, rows, 8):
            cos_at = pl.ds(i * PITCH + k, 8, stride=PITCH)
            sin_at = pl.ds(i * PITCH + k + ORDERS, 8, stride=PITCH)
            grid[cos_at, :] += value[i : i + 8, :mates]
            grid[sin_at, :] += value[i : i + 8, mates:]

    table = table_ref[...]

    def image_step(step, carry):
        base = pl.multiple_of(step * IMAGE_STEP, IMAGE_STEP)
        rows_out = []
        for i in range(0, IMAGE_STEP, 2):
            pieces = []
            for e in range(2):
                at = (base + i + e) * PITCH
                pieces.append(grid[pl.ds(at, 2 * ORDERS), :].astype(jnp.bfloat16))
            d = jnp.concatenate(pieces, axis=1)
            d = jnp.concatenate([d, d], axis=0)
            raw = jnp.dot(table, d, preferred_element_type=jnp.float32)
            top = jnp.max(raw, axis=0, keepdims=True)
            rows_out += [top[:, :mates], top[:, mates:]]
        best[pl.ds(base, IMAGE_STEP), :] = jnp.concatenate(rows_out, axis=0)
        return carry

    lax.fori_loop(0, rows // IMAGE_STEP, image_step, 0)

    def rms(ref, axis):
        x = ref[...].astype(jnp.float32)
        return jnp.sqrt(jnp.sum(x * x, axis=axis, keepdims=True) * (1.0 / cols) + 1e-06)

    scores = best[...] / (math.sqrt(cols) * rms(own_ref, 1) * rms(mate_ref, 0))
    best[...] = scores
    turned_ref[...] = scores.T
    share = mine_ref.shape[0]
    ang = lax.axis_index("ang")
    mine_ref[...] = best[pl.ds(pl.multiple_of(ang * share, share), share), :]
    if other_ref.shape[0] * 2 == rows:
        other_ref[...] = best[pl.ds(pl.multiple_of((1 - ang) * share, share), share), :]
    else:
        other_ref[...] = jnp.zeros_like(other_ref)


def per_device_wide(tables, coeffs, orders, plan):
    there, back = tables
    ang_count = lax.axis_size("ang")
    ang_index = lax.axis_index("ang")
    rows, cols = coeffs.shape
    share = rows // ang_count
    half = cols // 2
    blk_count = lax.axis_size("blk")
    low, high = jnp.minimum(plan[0], plan[1]), jnp.maximum(plan[0], plan[1])
    starts = jnp.sum(orders[None, :] < jnp.arange(ORDERS + 1)[:, None], axis=1).astype(jnp.int32)
    firsts = jnp.arange(half // LANES) * LANES
    heads = jnp.sum(starts[1:, None] <= firsts[None, :], axis=0).astype(jnp.int32)

    vmem = pl.BlockSpec(memory_space=pltpu.VMEM)
    smem = pl.BlockSpec(memory_space=pltpu.SMEM)
    params = pltpu.CompilerParams(vmem_limit_bytes=48 * 1024 * 1024)
    own, send, chosen = pl.pallas_call(
        sort_kernel,
        out_shape=(
            jax.ShapeDtypeStruct((rows, cols), jnp.bfloat16),
            jax.ShapeDtypeStruct((cols, share), jnp.bfloat16),
            jax.ShapeDtypeStruct((3,), jnp.int32),
        ),
        in_specs=[smem, vmem, pl.BlockSpec(memory_space=pltpu.HBM)],
        out_specs=(vmem, vmem, smem),
        scratch_shapes=[
            pltpu.VMEM((half, half), jnp.bfloat16),
            pltpu.VMEM((rows, cols), jnp.bfloat16),
            pltpu.SemaphoreType.DMA,
        ],
        compiler_params=params,
    )(plan, orders[None, :], coeffs)
    route, side, active = chosen[0], chosen[1], chosen[2]

    def over(value, choices, side_of_low):
        if len(choices) <= MOST_ROUTES:
            branches = [
                functools.partial(lambda pairs, v: lax.ppermute(v, "blk", pairs), pairs) for pairs in choices
            ]
            return lax.switch(route, branches, value)
        got = []
        for offset in (low, high):
            held = value
            for bit in range(blk_count.bit_length() - 1):
                pairs = [(b, b ^ (1 << bit)) for b in range(blk_count)]
                wanted = ((offset >> bit) & 1) == 1
                held = jnp.where(wanted, lax.ppermute(held, "blk", pairs), held)
            got.append(held)
        return jnp.where(side == side_of_low, got[0], got[1])

    mate = over(send, there, 1)
    wide = -(-share // LANES) * LANES
    mate = jnp.pad(mate, ((0, 0), (0, wide - share)))
    block = jax.ShapeDtypeStruct((share, wide), jnp.float32)
    mine, other, turned = pl.pallas_call(
        pair_kernel,
        out_shape=(block, block, jax.ShapeDtypeStruct((wide, rows), jnp.float32)),
        in_specs=[smem, smem, vmem, vmem, vmem],
        out_specs=(vmem, vmem, vmem),
        scratch_shapes=[
            pltpu.VMEM((rows * PITCH, wide), jnp.float32),
            pltpu.VMEM((rows, wide), jnp.float32),
        ],
        compiler_params=params,
    )(starts, heads, own, mate, jnp.asarray(angle_table()))
    sent = over(turned[:share], back, 0)
    if ang_count == 2:
        across = lax.ppermute(other, "ang", [(0, 1), (1, 0)])
        here = jnp.where(
            ang_index == 0,
            jnp.concatenate([mine, across], axis=1),
            jnp.concatenate([across, mine], axis=1),
        )
    else:
        pieces = turned[:share].T.reshape(ang_count, share, share)
        pieces = lax.all_to_all(pieces, "ang", 0, 0)
        here = pieces.transpose(1, 0, 2).reshape(share, rows)
    return jnp.where(
        active == 0, jnp.stack([here, sent]), jnp.stack([sent, here])
    )


MESH = pl.DeviceIdType.MESH
PRODUCTS = 8
IMAGES = 64


def slots_of(half):
    return ORDERS + half // LANES


def flipped(index, bits):
    for bit in range(bits.bit_length()):
        if (bits >> bit) & 1:
            index = index + (1 - 2 * bit_of(index, bit)) * (1 << bit)
    return index


def bit_of(index, bit):
    return lax.rem(lax.div(index, 1 << bit), 2)


def hail(devices):
    barrier = pltpu.get_barrier_semaphore()
    for device in devices:
        pl.semaphore_signal(barrier, inc=1, device_id=device, device_id_type=MESH)


def await_hails(devices):
    pl.semaphore_wait(pltpu.get_barrier_semaphore(), len(devices))


def greet(devices):
    hail(devices)
    await_hails(devices)


def remote(source, target, sent, arrived, device):
    return pltpu.make_async_remote_copy(
        src_ref=source,
        dst_ref=target,
        send_sem=sent,
        recv_sem=arrived,
        device_id=device,
        device_id_type=MESH,
    )


def swap_kernel(orders_hbm, table_hbm, plan_hbm, x_hbm, both_ref, perm_hbm, marks_ref, angles_ref, route_ref,
                flips_ref, orders_ref, table_ref, plan_ref, perm_ref, fetched, stored, sent, arrived):
    me = lax.axis_index("blk")
    sibling = {"blk": flipped(me, 1)}
    fetches = [
        pltpu.make_async_copy(source, target, fetched.at[n])
        for n, (source, target) in enumerate(
            [(orders_hbm, orders_ref), (plan_hbm, plan_ref), (table_hbm, table_ref), (x_hbm, both_ref.at[0])]
        )
    ]
    for fetch in fetches:
        fetch.start()
    greet([sibling])
    swap = remote(x_hbm, both_ref.at[1], sent, arrived, sibling)
    swap.start()
    for fetch in fetches[:3]:
        fetch.wait()
    route_ref[0] = (plan_ref[0] >> 1) * 256 + (plan_ref[1] >> 1)
    which = lax.broadcasted_iota(jnp.int32, flips_ref.shape, 0)
    even = jnp.where(which == 0, plan_ref[0], plan_ref[1]) & 1
    flips_ref[...] = 1.0 - even.astype(jnp.float32)

    half = orders_ref.shape[1]
    chunks = half // LANES
    slots = slots_of(half)
    orders = orders_ref[...].astype(jnp.float32)
    order = lax.broadcasted_iota(jnp.int32, (ORDERS, half), 0).astype(jnp.float32)
    ends = jnp.sum(jnp.where(orders <= order, 1.0, 0.0), axis=1, keepdims=True)

    def ended_before(place):
        return jnp.sum(jnp.where(ends <= place, 1.0, 0.0), axis=0, keepdims=True)

    def end_of(which):
        shape = (ORDERS, which.shape[1])
        row = lax.broadcasted_iota(jnp.int32, shape, 0).astype(jnp.float32)
        return jnp.sum(jnp.where(row == which, ends, 0.0), axis=0, keepdims=True)

    lane = lax.broadcasted_iota(jnp.int32, (1, LANES), 1).astype(jnp.float32)
    edge = (lane - ORDERS) * LANES
    late = lane >= ORDERS
    owner = jnp.where(late, ended_before(edge), lane)
    start, end = end_of(owner - 1), end_of(owner)
    chunk = jnp.zeros_like(lane)
    for c in range(1, chunks):
        chunk += jnp.where(start >= c * LANES, 1.0, 0.0)
    chunk = jnp.where(late, lane - ORDERS, chunk)
    low = jnp.where(late & (start >= edge), end, start) - chunk * LANES
    marks_ref[...] = jnp.concatenate([chunk, low, end - chunk * LANES], axis=0).astype(jnp.int32)

    wide = angles_ref.shape[1]
    place = lax.broadcasted_iota(jnp.int32, (1, wide), 1)
    part = sum(jnp.where(place >= slots * n, 1, 0) for n in range(1, 4))
    slot = (place - part * slots).astype(jnp.float32)
    wanted = jnp.where(slot < ORDERS, slot, ended_before((slot - ORDERS) * LANES))
    wanted = wanted + part.astype(jnp.float32) * ORDERS
    index = lax.broadcasted_iota(jnp.int32, (table_ref.shape[1], wide), 0).astype(jnp.float32)
    pick = jnp.where(index == wanted, 1.0, 0.0).astype(jnp.bfloat16)
    angles_ref[...] = jnp.dot(
        table_ref[...], pick, preferred_element_type=jnp.float32
    ).astype(jnp.bfloat16)

    spot = lax.broadcasted_iota(jnp.int32, (1, half), 1).astype(jnp.float32)
    key = orders * half + spot
    columns = [
        jnp.broadcast_to(key[:, c * LANES : (c + 1) * LANES], (LANES, LANES)).T for c in range(chunks)
    ]
    sub = lax.broadcasted_iota(jnp.int32, (half, LANES), 0).astype(jnp.float32)
    stores = [
        pltpu.make_async_copy(perm_ref.at[:, strip], perm_hbm.at[:, strip], stored.at[n])
        for n, strip in enumerate(pl.ds(n * LANES, LANES) for n in range(chunks))
    ]
    for d in range(chunks):
        piece = key[:, d * LANES : (d + 1) * LANES]
        count = jnp.zeros((LANES, LANES), jnp.float32)
        for c in range(chunks):
            count += jnp.where(columns[c] < piece, 1.0, 0.0)
        rank = jnp.sum(count, axis=0, keepdims=True)
        perm_ref[:, d * LANES : (d + 1) * LANES] = jnp.where(sub == rank, 1.0, 0.0).astype(jnp.bfloat16)
        if d:
            stores[d - 1].start()
    stores[-1].start()
    fetches[3].wait()
    swap.wait()
    for store in stores:
        store.wait()


def round_kernel(core, offset, flips_ref, marks_vmem, both_ref, perm_hbm, angles_ref, keep_ref, give_ref,
                 perm_ref, marks_ref, fetched, listed, local, offered, raw, own, mate, grid, best, scale, near, far, sent, arrived):
    me = lax.axis_index("blk")
    ang = lax.axis_index("ang")
    rows, cols = both_ref.shape[1:]
    half = cols // 2
    share = raw.shape[0]
    slots = slots_of(half)
    pitch = grid.shape[0] // rows
    width = 2 * LANES
    blocks = rows // IMAGES
    partner = {"blk": flipped(me, 2 * offset)}
    beside = {"ang": 1 - ang}

    def body():
        others = [partner, beside] if offset else [beside]
        hail(others)
        side = bit_of(me, low_bit(offset).bit_length()) if offset else 0
        swapped = flips_ref[core : core + 1, :1] * lax.convert_element_type(side, jnp.float32)
        flip = swapped.astype(jnp.bfloat16)
        stay = 1 - flip
        first = pl.multiple_of(ang * share, share)
        target = offered if offset else raw
        fetch = pltpu.make_async_copy(perm_hbm, perm_ref, fetched)
        fetch.start()
        listing = pltpu.make_async_copy(marks_vmem, marks_ref, listed)
        listing.start()

        def fill(step, carry):
            at = pl.multiple_of(step * 32, 32)
            here = pl.ds(first + at, 32)
            target[pl.ds(at, 32), :] = both_ref[0, here, :] * stay + both_ref[1, here, :] * flip
            return carry

        lax.fori_loop(0, share // 32, fill, 0)
        await_hails(others)
        if offset:
            offer = remote(offered, raw, sent.at[0], arrived.at[0], partner)
            offer.start()

        def norms(step, carry):
            here = pl.ds(pl.multiple_of(step * 32, 32), 32)
            x = both_ref[1, here, :] * stay + both_ref[0, here, :] * flip
            local[here, :] = x
            x = x.astype(jnp.float32)
            power = jnp.sum(x * x, axis=1, keepdims=True) * (1.0 / cols)
            rms = math.sqrt(cols) * jnp.sqrt(power + 1e-06)
            scale[here, :] = jnp.broadcast_to(1.0 / rms, (32, share))
            return carry

        lax.fori_loop(0, rows // 32, norms, 0)

        def sort_own(step, carry):
            d, part = lax.div(step, 2), lax.rem(step, 2)
            p = perm_ref[pl.ds(pl.multiple_of(d * width, width), width), :]
            x = local[:, pl.ds(pl.multiple_of(part * half, half), half)]
            got = lax.dot_general(x, p, NT, preferred_element_type=jnp.float32).astype(jnp.bfloat16)
            for e in range(2):
                own[2 * d + e, :, pl.ds(pl.multiple_of(part * LANES, LANES), LANES)] = got[
                    :, e * LANES : (e + 1) * LANES
                ]
            return carry

        fetch.wait()
        listing.wait()
        lax.fori_loop(0, cols // width, sort_own, 0)
        if offset:
            offer.wait()

        pair = jnp.concatenate([raw[:, :half], raw[:, half:]], axis=0)

        def sort_mates(step, carry):
            p = perm_ref[pl.ds(pl.multiple_of(step * 2 * width, 2 * width), 2 * width), :]
            got = lax.dot_general(p, pair, NT, preferred_element_type=jnp.float32)
            for e in range(4):
                mate[step * 4 + e] = got[e * LANES : (e + 1) * LANES].astype(jnp.bfloat16)
            return carry + jnp.sum(got * got, axis=0, keepdims=True)

        power = lax.fori_loop(
            0, half // (2 * width), sort_mates, jnp.zeros((1, 2 * share), jnp.float32)
        )
        power = (power[:, :share] + power[:, share:]) * (1.0 / cols)
        mates = 1.0 / jnp.sqrt(power + 1e-06)
        places = lax.broadcasted_iota(jnp.int32, (LANES, share), 0)

        def product(slot):
            chunk, low, high = marks_ref[0, slot], marks_ref[1, slot], marks_ref[2, slot]
            keep = jnp.where((places >= low) & (places < high), 1.0, 0.0).astype(jnp.bfloat16)
            uv = mate[chunk]
            u, v = uv[:, :share] * keep, uv[:, share:] * keep
            w = jnp.concatenate(
                [jnp.concatenate([u, v], axis=1), jnp.concatenate([v, -u], axis=1)], axis=0
            )
            return jnp.dot(own[chunk], w, preferred_element_type=jnp.float32)

        def products(step, carry):
            for e in range(PRODUCTS):
                slot = step * PRODUCTS + e
                value = product(slot)
                for i in range(0, rows, 8):
                    grid[pl.ds(i * pitch + slot, 8, stride=pitch), :] = value[i : i + 8, :share]
                    grid[pl.ds(i * pitch + slot + slots, 8, stride=pitch), :] = value[i : i + 8, share:]
            return carry

        lax.fori_loop(0, slots // PRODUCTS, products, 0)

        angles = angles_ref[:, : 4 * slots]
        early = blocks // 2

        def base_of(step):
            return pl.multiple_of(lax.rem(step + early * (1 - ang), blocks) * IMAGES, IMAGES)

        def back(step):
            piece = pl.ds(base_of(step), IMAGES)
            return remote(best.at[piece, :], far.at[piece, :], sent.at[1 + step], arrived.at[1 + step], partner)

        def across(step):
            return remote(
                best.at[pl.ds(base_of(step), IMAGES), :],
                near.at[pl.ds(pl.multiple_of(step * IMAGES, IMAGES), IMAGES), :],
                sent.at[1 + blocks + step],
                arrived.at[1 + blocks + step],
                beside,
            )

        def ship(step):
            if offset:
                back(step).start()
            pl.when(step < early)(lambda: across(step).start())

        def images(step, carry):
            base = base_of(step)
            tops = []
            for i in range(0, IMAGES, 2):
                pieces = [
                    grid[pl.ds((base + i + e) * pitch, 2 * slots), :].astype(jnp.bfloat16) for e in range(2)
                ]
                d = jnp.concatenate(pieces, axis=1)
                d = jnp.concatenate([d, d], axis=0)
                score = jnp.dot(angles, d, preferred_element_type=jnp.float32)
                top = jnp.max(score, axis=0, keepdims=True)
                tops += [top[:, :share], top[:, share:]]
            top = jnp.concatenate(tops, axis=0)
            best[pl.ds(base, IMAGES), :] = top * scale[pl.ds(base, IMAGES), :] * mates
            pl.when(step > 0)(lambda: ship(step - 1))
            return carry

        lax.fori_loop(0, blocks, images, 0)
        ship(blocks - 1)
        for step in range(early):
            across(step).wait()
        mine, other = best[pl.ds(first, share), :], near[...]
        ahead = lax.broadcasted_iota(jnp.int32, (share, share), 0) * 0 + ang == 0
        here = jnp.concatenate(
            [jnp.where(ahead, mine, other), jnp.where(ahead, other, mine)], axis=1
        )
        if offset:
            for step in range(blocks):
                back(step).wait()
            there = far[...].T
        else:
            there = best[...].T
        local_own = jnp.broadcast_to(swapped, (share, rows)) > 0.5
        keep_ref[...] = jnp.where(local_own, here, there)
        give_ref[...] = jnp.where(local_own, there, here)

    pl.when(bit_of(me, 0) == core)(body)


def last_kernel(keep_0, give_0, keep_1, give_1, out_ref, sent, arrived):
    me = lax.axis_index("blk")
    sibling = {"blk": flipped(me, 1)}
    greet([sibling])

    def finish(core, keep, give):
        def body():
            copy = remote(give, out_ref.at[core], sent, arrived, sibling)
            copy.start()
            out_ref[core] = keep[...]
            copy.wait_send()
            remote(give, out_ref.at[1 - core], sent, arrived, sibling).wait_recv()

        pl.when(bit_of(me, 0) == core)(body)

    finish(0, keep_0, give_0)
    finish(1, keep_1, give_1)


def per_device(coeffs, orders, plan):
    rows, cols = coeffs.shape
    share = rows // lax.axis_size("ang")
    half = cols // 2
    chips = lax.axis_size("blk") // 2
    slots = slots_of(half)
    wide = -(-4 * slots // LANES) * LANES
    vmem = pl.BlockSpec(memory_space=pltpu.VMEM)
    smem = pl.BlockSpec(memory_space=pltpu.SMEM)
    hbm = pl.BlockSpec(memory_space=pltpu.HBM)

    def params(number, mib):
        return pltpu.CompilerParams(
            has_side_effects=True, collective_id=number, vmem_limit_bytes=mib * 1024 * 1024
        )

    far_off = functools.partial(pltpu.with_memory_space_constraint, memory_space=pltpu.HBM)
    table = angle_table()
    number = jax.ShapeDtypeStruct((1,), jnp.int32)
    both, perm, marks, angles, routes, flips = pl.pallas_call(
        swap_kernel,
        out_shape=(
            jax.ShapeDtypeStruct((2, rows, cols), jnp.bfloat16),
            pltpu.HBM((half, half), jnp.bfloat16),
            jax.ShapeDtypeStruct((3, LANES), jnp.int32),
            jax.ShapeDtypeStruct((ANGLES, wide), jnp.bfloat16),
            number,
            jax.ShapeDtypeStruct((8, LANES), jnp.float32),
        ),
        in_specs=[hbm] * 4,
        out_specs=(vmem, hbm, vmem, vmem, smem, vmem),
        scratch_shapes=[
            pltpu.VMEM((1, half), jnp.int32),
            pltpu.VMEM(table.shape, jnp.bfloat16),
            pltpu.SMEM((ROUNDS,), jnp.int32),
            pltpu.VMEM((half, half), jnp.bfloat16),
            pltpu.SemaphoreType.DMA((4,)),
            pltpu.SemaphoreType.DMA((half // LANES,)),
            pltpu.SemaphoreType.DMA,
            pltpu.SemaphoreType.DMA,
        ],
        compiler_params=params(0, 6),
    )(*[far_off(value) for value in (orders[None, :], jnp.asarray(table), plan, coeffs)])

    result = jax.ShapeDtypeStruct((share, rows), jnp.float32)
    copies = 1 + rows // IMAGES + share // IMAGES
    found = []
    for core, route in enumerate((routes[0] >> 8, routes[0] & 255)):
        rounds = [
            pl.pallas_call(
                functools.partial(round_kernel, core, offset),
                out_shape=(result, result),
                in_specs=[vmem, vmem, vmem, hbm, vmem],
                out_specs=(vmem, vmem),
                scratch_shapes=[
                    pltpu.VMEM((half, half), jnp.bfloat16),
                    pltpu.SMEM((3, LANES), jnp.int32),
                    pltpu.SemaphoreType.DMA,
                    pltpu.SemaphoreType.DMA,
                    pltpu.VMEM((rows, cols), jnp.bfloat16),
                    pltpu.VMEM((share, cols), jnp.bfloat16),
                    pltpu.VMEM((share, cols), jnp.bfloat16),
                    pltpu.VMEM((half // LANES, rows, 2 * LANES), jnp.bfloat16),
                    pltpu.VMEM((half // LANES, LANES, 2 * share), jnp.bfloat16),
                    pltpu.VMEM((rows * (2 * slots + 1), share), jnp.float32),
                    pltpu.VMEM((rows, share), jnp.float32),
                    pltpu.VMEM((rows, share), jnp.float32),
                    pltpu.VMEM((share, share), jnp.float32),
                    pltpu.VMEM((rows, share), jnp.float32),
                    pltpu.SemaphoreType.DMA((copies,)),
                    pltpu.SemaphoreType.DMA((copies,)),
                ],
                compiler_params=params(1 + core * chips + offset, 26),
            )
            for offset in range(chips)
        ]
        found += lax.switch(route, rounds, flips, marks, both, perm, angles)
    return pl.pallas_call(
        last_kernel,
        out_shape=jax.ShapeDtypeStruct((ROUNDS, share, rows), jnp.float32),
        in_specs=[vmem] * 4,
        out_specs=vmem,
        scratch_shapes=[pltpu.SemaphoreType.DMA] * 2,
        compiler_params=params(1 + 2 * chips, 8),
    )(*found)


def solution(mesh):
    n_blk, n_ang = mesh.shape["blk"], mesh.shape["ang"]
    body = per_device if n_blk <= 16 and n_ang == 2 else functools.partial(per_device_wide, routes(n_blk))
    return jax.shard_map(
        body,
        mesh=mesh,
        in_specs=(P("blk", None), P(), P()),
        out_specs=P(None, ("blk", "ang"), None),
        check_vma=False,
    )
```

```python
import functools
import math

import jax
import jax.numpy as jnp
import numpy as np
from jax import lax
from jax.experimental import pallas as pl
from jax.experimental.pallas import tpu as pltpu
from jax.sharding import PartitionSpec as P

ANGLES = 128
ORDERS = 48
ROUNDS = 2
LANES = 128
PITCH = 97
ORDER_STEP = 16
IMAGE_STEP = 64
MOST_ROUTES = 128
NT = (((1,), (1,)), ((), ()))


def low_bit(value):
    return value & -value


def side_mask(p, q):
    both = p & q
    plain = jnp.where(both != 0, low_bit(both), low_bit(p) | low_bit(q))
    odd, even = jnp.where(p & 1, p, q), jnp.where(p & 1, q, p)
    rest = even & ~odd
    mixed = jnp.where(rest != 0, 1 | low_bit(rest), plain)
    return jnp.where(both & 1, 1, jnp.where((p | q) & 1, mixed, plain | 1))


def parity(value, bits):
    return sum((value >> bit) & 1 for bit in range(bits)) & 1


def side_mask_of(p, q):
    low = lambda v: v & -v
    both = p & q
    plain = low(both) if both else low(p) | low(q)
    if both & 1:
        return 1
    if (p | q) & 1:
        odd, even = (p, q) if p & 1 else (q, p)
        rest = even & ~odd
        return 1 | low(rest) if rest else plain
    return plain | 1


def routes(n_blk):
    there, back = [], []
    for p in range(1, n_blk):
        for q in range(p, n_blk):
            mask = side_mask_of(p, q)
            assert bin(mask & p).count("1") % 2 and bin(mask & q).count("1") % 2
            pairs = [(b, b ^ (q if bin(mask & b).count("1") % 2 else p)) for b in range(n_blk)]
            assert sorted(t for _, t in pairs) == list(range(n_blk))
            there.append(pairs)
            back.append([(t, s) for s, t in pairs])
    return there, back


def angle_table():
    theta = 2.0 * math.pi * np.arange(ANGLES) / ANGLES
    phase = theta[:, None] * np.arange(ORDERS)[None, :]
    full = np.concatenate([np.cos(phase), np.sin(phase)], axis=1)
    high = full.astype(np.float32).astype(jnp.bfloat16)
    low = (full - high.astype(np.float64)).astype(np.float32).astype(jnp.bfloat16)
    return np.concatenate([high, low], axis=1)


def sort_kernel(plan_ref, orders_ref, x_hbm, own_ref, send_ref, route_ref, perm, x_ref, arrived):
    fetch = pltpu.make_async_copy(x_hbm, x_ref, arrived)
    fetch.start()
    blk_count = lax.axis_size("blk")
    low, high = jnp.minimum(plan_ref[0], plan_ref[1]), jnp.maximum(plan_ref[0], plan_ref[1])
    side = parity(side_mask(low, high) & lax.axis_index("blk"), blk_count.bit_length() - 1)
    route_ref[0] = (low - 1) * blk_count - (((low - 1) * low) >> 1) + high - low
    route_ref[1] = side
    route_ref[2] = (1 - side) ^ jnp.where(plan_ref[0] > plan_ref[1], 1, 0)
    half = orders_ref.shape[1]
    chunks = half // LANES
    slot = lax.broadcasted_iota(jnp.int32, (1, half), 1)
    key = (orders_ref[...] * half + slot).astype(jnp.float32)
    lane = lax.broadcasted_iota(jnp.int32, (LANES, half), 1).astype(jnp.float32)
    for c in range(chunks):
        piece = key[:, c * LANES : (c + 1) * LANES]
        column = jnp.broadcast_to(piece, (LANES, LANES)).T
        count = jnp.zeros((LANES, LANES), jnp.float32)
        for d in range(chunks):
            other = key[:, d * LANES : (d + 1) * LANES]
            count += jnp.where(other < column, 1.0, 0.0)
        rank = jnp.sum(count, axis=1, keepdims=True)
        perm[c * LANES : (c + 1) * LANES, :] = jnp.where(lane == rank, 1.0, 0.0).astype(jnp.bfloat16)
    fetch.wait()
    width = 2 * LANES
    for d in range(half // width):
        p = perm[:, d * width : (d + 1) * width]
        for part in range(2):
            got = jnp.dot(
                x_ref[:, part * half : (part + 1) * half], p, preferred_element_type=jnp.float32
            ).astype(jnp.bfloat16)
            for e in range(2):
                at = ((2 * d + e) * 2 + part) * LANES
                own_ref[:, at : at + LANES] = got[:, e * LANES : (e + 1) * LANES]
    share = send_ref.shape[1]
    first = pl.multiple_of(lax.axis_index("ang") * share, share)
    for at in range(0, 2 * half, LANES):
        send_ref[at : at + LANES, :] = own_ref[pl.ds(first, share), at : at + LANES].T


def pair_kernel(starts, heads, own_ref, mate_ref, table_ref, mine_ref, other_ref, turned_ref, grid, best):
    rows, cols = own_ref.shape
    mates = mate_ref.shape[1]
    width = 2 * LANES
    slots = lax.broadcasted_iota(jnp.int32, (LANES, mates), 0)

    def product(chunk, low, high):
        at = chunk * width if isinstance(chunk, int) else pl.multiple_of(chunk * width, width)
        place = slots + chunk * LANES
        keep = jnp.where((place >= low) & (place < high), 1.0, 0.0).astype(jnp.bfloat16)
        u = mate_ref[pl.ds(at, LANES), :] * keep
        v = mate_ref[pl.ds(at + LANES, LANES), :] * keep
        w = jnp.concatenate(
            [jnp.concatenate([u, v], axis=1), jnp.concatenate([v, -u], axis=1)], axis=0
        )
        return jnp.dot(own_ref[:, pl.ds(at, width)], w, preferred_element_type=jnp.float32)

    def spread(k, value):
        for i in range(0, rows, 8):
            grid[pl.ds(i * PITCH + k, 8, stride=PITCH), :] = value[i : i + 8, :mates]
            grid[pl.ds(i * PITCH + k + ORDERS, 8, stride=PITCH), :] = value[i : i + 8, mates:]

    def first_chunks(step, carry):
        for e in range(ORDER_STEP):
            k = step * ORDER_STEP + e
            low = starts[k]
            spread(k, product(jnp.minimum(low // LANES, cols // width - 1), low, starts[k + 1]))
        return carry

    lax.fori_loop(0, ORDERS // ORDER_STEP, first_chunks, 0)

    for chunk in range(1, cols // width):
        k = heads[chunk]
        low = jnp.where(starts[k] < chunk * LANES, starts[k], starts[k + 1])
        value = product(chunk, low, starts[k + 1])
        for i in range(0, rows, 8):
            cos_at = pl.ds(i * PITCH + k, 8, stride=PITCH)
            sin_at = pl.ds(i * PITCH + k + ORDERS, 8, stride=PITCH)
            grid[cos_at, :] += value[i : i + 8, :mates]
            grid[sin_at, :] += value[i : i + 8, mates:]

    table = table_ref[...]

    def image_step(step, carry):
        base = pl.multiple_of(step * IMAGE_STEP, IMAGE_STEP)
        rows_out = []
        for i in range(0, IMAGE_STEP, 2):
            pieces = []
            for e in range(2):
                at = (base + i + e) * PITCH
                pieces.append(grid[pl.ds(at, 2 * ORDERS), :].astype(jnp.bfloat16))
            d = jnp.concatenate(pieces, axis=1)
            d = jnp.concatenate([d, d], axis=0)
            raw = jnp.dot(table, d, preferred_element_type=jnp.float32)
            top = jnp.max(raw, axis=0, keepdims=True)
            rows_out += [top[:, :mates], top[:, mates:]]
        best[pl.ds(base, IMAGE_STEP), :] = jnp.concatenate(rows_out, axis=0)
        return carry

    lax.fori_loop(0, rows // IMAGE_STEP, image_step, 0)

    def rms(ref, axis):
        x = ref[...].astype(jnp.float32)
        return jnp.sqrt(jnp.sum(x * x, axis=axis, keepdims=True) * (1.0 / cols) + 1e-06)

    scores = best[...] / (math.sqrt(cols) * rms(own_ref, 1) * rms(mate_ref, 0))
    best[...] = scores
    turned_ref[...] = scores.T
    share = mine_ref.shape[0]
    ang = lax.axis_index("ang")
    mine_ref[...] = best[pl.ds(pl.multiple_of(ang * share, share), share), :]
    if other_ref.shape[0] * 2 == rows:
        other_ref[...] = best[pl.ds(pl.multiple_of((1 - ang) * share, share), share), :]
    else:
        other_ref[...] = jnp.zeros_like(other_ref)


def per_device_wide(tables, coeffs, orders, plan):
    there, back = tables
    ang_count = lax.axis_size("ang")
    ang_index = lax.axis_index("ang")
    rows, cols = coeffs.shape
    share = rows // ang_count
    half = cols // 2
    blk_count = lax.axis_size("blk")
    low, high = jnp.minimum(plan[0], plan[1]), jnp.maximum(plan[0], plan[1])
    starts = jnp.sum(orders[None, :] < jnp.arange(ORDERS + 1)[:, None], axis=1).astype(jnp.int32)
    firsts = jnp.arange(half // LANES) * LANES
    heads = jnp.sum(starts[1:, None] <= firsts[None, :], axis=0).astype(jnp.int32)

    vmem = pl.BlockSpec(memory_space=pltpu.VMEM)
    smem = pl.BlockSpec(memory_space=pltpu.SMEM)
    params = pltpu.CompilerParams(vmem_limit_bytes=48 * 1024 * 1024)
    own, send, chosen = pl.pallas_call(
        sort_kernel,
        out_shape=(
            jax.ShapeDtypeStruct((rows, cols), jnp.bfloat16),
            jax.ShapeDtypeStruct((cols, share), jnp.bfloat16),
            jax.ShapeDtypeStruct((3,), jnp.int32),
        ),
        in_specs=[smem, vmem, pl.BlockSpec(memory_space=pltpu.HBM)],
        out_specs=(vmem, vmem, smem),
        scratch_shapes=[
            pltpu.VMEM((half, half), jnp.bfloat16),
            pltpu.VMEM((rows, cols), jnp.bfloat16),
            pltpu.SemaphoreType.DMA,
        ],
        compiler_params=params,
    )(plan, orders[None, :], coeffs)
    route, side, active = chosen[0], chosen[1], chosen[2]

    def over(value, choices, side_of_low):
        if len(choices) <= MOST_ROUTES:
            branches = [
                functools.partial(lambda pairs, v: lax.ppermute(v, "blk", pairs), pairs) for pairs in choices
            ]
            return lax.switch(route, branches, value)
        got = []
        for offset in (low, high):
            held = value
            for bit in range(blk_count.bit_length() - 1):
                pairs = [(b, b ^ (1 << bit)) for b in range(blk_count)]
                wanted = ((offset >> bit) & 1) == 1
                held = jnp.where(wanted, lax.ppermute(held, "blk", pairs), held)
            got.append(held)
        return jnp.where(side == side_of_low, got[0], got[1])

    mate = over(send, there, 1)
    wide = -(-share // LANES) * LANES
    mate = jnp.pad(mate, ((0, 0), (0, wide - share)))
    block = jax.ShapeDtypeStruct((share, wide), jnp.float32)
    mine, other, turned = pl.pallas_call(
        pair_kernel,
        out_shape=(block, block, jax.ShapeDtypeStruct((wide, rows), jnp.float32)),
        in_specs=[smem, smem, vmem, vmem, vmem],
        out_specs=(vmem, vmem, vmem),
        scratch_shapes=[
            pltpu.VMEM((rows * PITCH, wide), jnp.float32),
            pltpu.VMEM((rows, wide), jnp.float32),
        ],
        compiler_params=params,
    )(starts, heads, own, mate, jnp.asarray(angle_table()))
    sent = over(turned[:share], back, 0)
    if ang_count == 2:
        across = lax.ppermute(other, "ang", [(0, 1), (1, 0)])
        here = jnp.where(
            ang_index == 0,
            jnp.concatenate([mine, across], axis=1),
            jnp.concatenate([across, mine], axis=1),
        )
    else:
        pieces = turned[:share].T.reshape(ang_count, share, share)
        pieces = lax.all_to_all(pieces, "ang", 0, 0)
        here = pieces.transpose(1, 0, 2).reshape(share, rows)
    return jnp.where(
        active == 0, jnp.stack([here, sent]), jnp.stack([sent, here])
    )


MESH = pl.DeviceIdType.MESH
PRODUCTS = 14
IMAGES = 32


def slots_of(half):
    return ORDERS + half // LANES


def flipped(index, bits):
    for bit in range(bits.bit_length()):
        if (bits >> bit) & 1:
            index = index + (1 - 2 * bit_of(index, bit)) * (1 << bit)
    return index


def bit_of(index, bit):
    return lax.rem(lax.div(index, 1 << bit), 2)


def hail(devices):
    barrier = pltpu.get_barrier_semaphore()
    for device in devices:
        pl.semaphore_signal(barrier, inc=1, device_id=device, device_id_type=MESH)


def await_hails(devices):
    pl.semaphore_wait(pltpu.get_barrier_semaphore(), len(devices))


def greet(devices):
    hail(devices)
    await_hails(devices)


def remote(source, target, sent, arrived, device):
    return pltpu.make_async_remote_copy(
        src_ref=source,
        dst_ref=target,
        send_sem=sent,
        recv_sem=arrived,
        device_id=device,
        device_id_type=MESH,
    )


def swap_kernel(orders_hbm, table_hbm, plan_hbm, x_hbm, both_ref, perm_hbm, marks_ref, angles_ref, route_ref,
                flips_ref, orders_ref, table_ref, plan_ref, perm_ref, fetched, stored, sent, arrived):
    me = lax.axis_index("blk")
    sibling = {"blk": flipped(me, 1)}
    fetches = [
        pltpu.make_async_copy(source, target, fetched.at[n])
        for n, (source, target) in enumerate(
            [(orders_hbm, orders_ref), (plan_hbm, plan_ref), (table_hbm, table_ref), (x_hbm, both_ref.at[0])]
        )
    ]
    for fetch in fetches:
        fetch.start()
    greet([sibling])
    swap = remote(x_hbm, both_ref.at[1], sent, arrived, sibling)
    swap.start()
    fetches[0].wait()
    half = orders_ref.shape[1]
    chunks = half // LANES
    slots = slots_of(half)
    orders = orders_ref[...].astype(jnp.float32)
    spot = lax.broadcasted_iota(jnp.int32, (1, half), 1).astype(jnp.float32)
    key = orders * half + spot
    columns = [
        jnp.broadcast_to(key[:, c * LANES : (c + 1) * LANES], (LANES, LANES)).T for c in range(chunks)
    ]
    sub = lax.broadcasted_iota(jnp.int32, (half, LANES), 0).astype(jnp.float32)
    stores = [
        pltpu.make_async_copy(perm_ref.at[:, strip], perm_hbm.at[:, strip], stored.at[n])
        for n, strip in enumerate(pl.ds(n * LANES, LANES) for n in range(chunks))
    ]
    for d in range(chunks):
        piece = key[:, d * LANES : (d + 1) * LANES]
        count = jnp.zeros((LANES, LANES), jnp.float32)
        for c in range(chunks):
            count += jnp.where(columns[c] < piece, 1.0, 0.0)
        rank = jnp.sum(count, axis=0, keepdims=True)
        perm_ref[:, d * LANES : (d + 1) * LANES] = jnp.where(sub == rank, 1.0, 0.0).astype(jnp.bfloat16)
        if d:
            stores[d - 1].start()
    stores[-1].start()

    for fetch in fetches[1:3]:
        fetch.wait()
    route_ref[0] = (plan_ref[0] >> 1) * 256 + (plan_ref[1] >> 1)
    which = lax.broadcasted_iota(jnp.int32, flips_ref.shape, 0)
    even = jnp.where(which == 0, plan_ref[0], plan_ref[1]) & 1
    flips_ref[...] = 1.0 - even.astype(jnp.float32)
    order = lax.broadcasted_iota(jnp.int32, (ORDERS, half), 0).astype(jnp.float32)
    ends = jnp.sum(jnp.where(orders <= order, 1.0, 0.0), axis=1, keepdims=True)

    def ended_before(place):
        return jnp.sum(jnp.where(ends <= place, 1.0, 0.0), axis=0, keepdims=True)

    def end_of(which):
        shape = (ORDERS, which.shape[1])
        row = lax.broadcasted_iota(jnp.int32, shape, 0).astype(jnp.float32)
        return jnp.sum(jnp.where(row == which, ends, 0.0), axis=0, keepdims=True)

    lane = lax.broadcasted_iota(jnp.int32, (1, LANES), 1).astype(jnp.float32)
    edge = (lane - ORDERS) * LANES
    late = lane >= ORDERS
    owner = jnp.where(late, ended_before(edge), lane)
    start, end = end_of(owner - 1), end_of(owner)
    chunk = jnp.zeros_like(lane)
    for c in range(1, chunks):
        chunk += jnp.where(start >= c * LANES, 1.0, 0.0)
    chunk = jnp.where(late, lane - ORDERS, chunk)
    low = jnp.where(late & (start >= edge), end, start) - chunk * LANES
    marks_ref[...] = jnp.concatenate([chunk, low, end - chunk * LANES], axis=0).astype(jnp.int32)

    wide = angles_ref.shape[1]
    place = lax.broadcasted_iota(jnp.int32, (1, wide), 1)
    part = sum(jnp.where(place >= slots * n, 1, 0) for n in range(1, 4))
    slot = (place - part * slots).astype(jnp.float32)
    wanted = jnp.where(slot < ORDERS, slot, ended_before((slot - ORDERS) * LANES))
    wanted = wanted + part.astype(jnp.float32) * ORDERS
    index = lax.broadcasted_iota(jnp.int32, (table_ref.shape[1], wide), 0).astype(jnp.float32)
    pick = jnp.where(index == wanted, 1.0, 0.0).astype(jnp.bfloat16)
    angles_ref[...] = jnp.dot(
        table_ref[...], pick, preferred_element_type=jnp.float32
    ).astype(jnp.bfloat16)

    fetches[3].wait()
    swap.wait()
    for store in stores:
        store.wait()


def round_kernel(core, offset, flips_ref, marks_vmem, both_ref, perm_hbm, angles_ref, keep_ref, give_ref,
                 perm_ref, marks_ref, fetched, listed, local, offered, raw, own, mate, grid, best, scale, near, far, sent, arrived):
    me = lax.axis_index("blk")
    ang = lax.axis_index("ang")
    rows, cols = both_ref.shape[1:]
    half = cols // 2
    share = raw.shape[0]
    slots = slots_of(half)
    pitch = grid.shape[0] // rows
    width = 2 * LANES
    blocks = rows // IMAGES
    partner = {"blk": flipped(me, 2 * offset)}
    beside = {"ang": 1 - ang}

    def body():
        others = [partner, beside] if offset else [beside]
        hail(others)
        side = bit_of(me, low_bit(offset).bit_length()) if offset else 0
        swapped = flips_ref[core : core + 1, :1] * lax.convert_element_type(side, jnp.float32)
        flip = swapped.astype(jnp.bfloat16)
        stay = 1 - flip
        first = pl.multiple_of(ang * share, share)
        target = offered if offset else raw
        fetch = pltpu.make_async_copy(perm_hbm, perm_ref, fetched)
        fetch.start()
        listing = pltpu.make_async_copy(marks_vmem, marks_ref, listed)
        listing.start()

        def fill(step, carry):
            at = pl.multiple_of(step * 32, 32)
            here = pl.ds(first + at, 32)
            target[pl.ds(at, 32), :] = both_ref[0, here, :] * stay + both_ref[1, here, :] * flip
            return carry

        lax.fori_loop(0, share // 32, fill, 0)
        await_hails(others)
        if offset:
            offer = remote(offered, raw, sent.at[0], arrived.at[0], partner)
            offer.start()

        def norms(step, carry):
            here = pl.ds(pl.multiple_of(step * 32, 32), 32)
            x = both_ref[1, here, :] * stay + both_ref[0, here, :] * flip
            local[here, :] = x
            x = x.astype(jnp.float32)
            power = jnp.sum(x * x, axis=1, keepdims=True) * (1.0 / cols)
            rms = math.sqrt(cols) * jnp.sqrt(power + 1e-06)
            scale[here, :] = jnp.broadcast_to(1.0 / rms, (32, share))
            return carry

        lax.fori_loop(0, rows // 32, norms, 0)

        def sort_own(step, carry):
            d, part = lax.div(step, 2), lax.rem(step, 2)
            p = perm_ref[pl.ds(pl.multiple_of(d * width, width), width), :]
            x = local[:, pl.ds(pl.multiple_of(part * half, half), half)]
            got = lax.dot_general(x, p, NT, preferred_element_type=jnp.float32).astype(jnp.bfloat16)
            for e in range(2):
                own[2 * d + e, :, pl.ds(pl.multiple_of(part * LANES, LANES), LANES)] = got[
                    :, e * LANES : (e + 1) * LANES
                ]
            return carry

        fetch.wait()
        listing.wait()
        lax.fori_loop(0, cols // width, sort_own, 0)
        if offset:
            offer.wait()

        pair = jnp.concatenate([raw[:, :half], raw[:, half:]], axis=0)

        def sort_mates(step, carry):
            p = perm_ref[pl.ds(pl.multiple_of(step * 2 * width, 2 * width), 2 * width), :]
            got = lax.dot_general(p, pair, NT, preferred_element_type=jnp.float32)
            for e in range(4):
                mate[step * 4 + e] = got[e * LANES : (e + 1) * LANES].astype(jnp.bfloat16)
            return carry + jnp.sum(got * got, axis=0, keepdims=True)

        power = lax.fori_loop(
            0, half // (2 * width), sort_mates, jnp.zeros((1, 2 * share), jnp.float32)
        )
        power = (power[:, :share] + power[:, share:]) * (1.0 / cols)
        mates = 1.0 / jnp.sqrt(power + 1e-06)
        places = lax.broadcasted_iota(jnp.int32, (LANES, share), 0)

        def product(slot):
            chunk, low, high = marks_ref[0, slot], marks_ref[1, slot], marks_ref[2, slot]
            keep = jnp.where((places >= low) & (places < high), 1.0, 0.0).astype(jnp.bfloat16)
            uv = mate[chunk]
            u, v = uv[:, :share] * keep, uv[:, share:] * keep
            w = jnp.concatenate(
                [jnp.concatenate([u, v], axis=1), jnp.concatenate([v, -u], axis=1)], axis=0
            )
            return jnp.dot(own[chunk], w, preferred_element_type=jnp.float32)

        def products(step, carry):
            for e in range(PRODUCTS):
                slot = step * PRODUCTS + e
                value = product(slot)
                for i in range(0, rows, 8):
                    grid[pl.ds(i * pitch + slot, 8, stride=pitch), :] = value[i : i + 8, :share]
                    grid[pl.ds(i * pitch + slot + slots, 8, stride=pitch), :] = value[i : i + 8, share:]
            return carry

        lax.fori_loop(0, slots // PRODUCTS, products, 0)

        angles = angles_ref[:, : 4 * slots]
        early = blocks // 2

        def base_of(step):
            return pl.multiple_of(lax.rem(step + early * (1 - ang), blocks) * IMAGES, IMAGES)

        def back(step):
            piece = pl.ds(base_of(step), IMAGES)
            return remote(best.at[piece, :], far.at[piece, :], sent.at[1 + step], arrived.at[1 + step], partner)

        def across(step):
            return remote(
                best.at[pl.ds(base_of(step), IMAGES), :],
                near.at[pl.ds(pl.multiple_of(step * IMAGES, IMAGES), IMAGES), :],
                sent.at[1 + blocks + step],
                arrived.at[1 + blocks + step],
                beside,
            )

        def ship(step):
            if offset:
                back(step).start()
            pl.when(step < early)(lambda: across(step).start())

        def images(step, carry):
            base = base_of(step)
            tops = []
            for i in range(0, IMAGES, 2):
                pieces = [
                    grid[pl.ds((base + i + e) * pitch, 2 * slots), :].astype(jnp.bfloat16) for e in range(2)
                ]
                d = jnp.concatenate(pieces, axis=1)
                d = jnp.concatenate([d, d], axis=0)
                score = jnp.dot(angles, d, preferred_element_type=jnp.float32)
                top = jnp.max(score, axis=0, keepdims=True)
                tops += [top[:, :share], top[:, share:]]
            top = jnp.concatenate(tops, axis=0)
            best[pl.ds(base, IMAGES), :] = top * scale[pl.ds(base, IMAGES), :] * mates
            pl.when(step > 0)(lambda: ship(step - 1))
            return carry

        lax.fori_loop(0, blocks, images, 0)
        ship(blocks - 1)
        for step in range(early):
            across(step).wait()
        mine, other = best[pl.ds(first, share), :], near[...]
        ahead = lax.broadcasted_iota(jnp.int32, (share, share), 0) * 0 + ang == 0
        here = jnp.concatenate(
            [jnp.where(ahead, mine, other), jnp.where(ahead, other, mine)], axis=1
        )
        if offset:
            for step in range(blocks):
                back(step).wait()
            there = far[...].T
        else:
            there = best[...].T
        local_own = jnp.broadcast_to(swapped, (share, rows)) > 0.5
        keep_ref[...] = jnp.where(local_own, here, there)
        give_ref[...] = jnp.where(local_own, there, here)

    pl.when(bit_of(me, 0) == core)(body)


def last_kernel(keep_0, give_0, keep_1, give_1, out_ref, sent, arrived):
    me = lax.axis_index("blk")
    sibling = {"blk": flipped(me, 1)}
    greet([sibling])

    def finish(core, keep, give):
        def body():
            copy = remote(give, out_ref.at[core], sent, arrived, sibling)
            copy.start()
            out_ref[core] = keep[...]
            copy.wait_send()
            remote(give, out_ref.at[1 - core], sent, arrived, sibling).wait_recv()

        pl.when(bit_of(me, 0) == core)(body)

    finish(0, keep_0, give_0)
    finish(1, keep_1, give_1)


def per_device(coeffs, orders, plan):
    rows, cols = coeffs.shape
    share = rows // lax.axis_size("ang")
    half = cols // 2
    chips = lax.axis_size("blk") // 2
    slots = slots_of(half)
    wide = -(-4 * slots // LANES) * LANES
    vmem = pl.BlockSpec(memory_space=pltpu.VMEM)
    smem = pl.BlockSpec(memory_space=pltpu.SMEM)
    hbm = pl.BlockSpec(memory_space=pltpu.HBM)

    def params(number, mib):
        return pltpu.CompilerParams(
            has_side_effects=True, collective_id=number, vmem_limit_bytes=mib * 1024 * 1024
        )

    far_off = functools.partial(pltpu.with_memory_space_constraint, memory_space=pltpu.HBM)
    table = angle_table()
    number = jax.ShapeDtypeStruct((1,), jnp.int32)
    both, perm, marks, angles, routes, flips = pl.pallas_call(
        swap_kernel,
        out_shape=(
            jax.ShapeDtypeStruct((2, rows, cols), jnp.bfloat16),
            pltpu.HBM((half, half), jnp.bfloat16),
            jax.ShapeDtypeStruct((3, LANES), jnp.int32),
            jax.ShapeDtypeStruct((ANGLES, wide), jnp.bfloat16),
            number,
            jax.ShapeDtypeStruct((8, LANES), jnp.float32),
        ),
        in_specs=[hbm] * 4,
        out_specs=(vmem, hbm, vmem, vmem, smem, vmem),
        scratch_shapes=[
            pltpu.VMEM((1, half), jnp.int32),
            pltpu.VMEM(table.shape, jnp.bfloat16),
            pltpu.SMEM((ROUNDS,), jnp.int32),
            pltpu.VMEM((half, half), jnp.bfloat16),
            pltpu.SemaphoreType.DMA((4,)),
            pltpu.SemaphoreType.DMA((half // LANES,)),
            pltpu.SemaphoreType.DMA,
            pltpu.SemaphoreType.DMA,
        ],
        compiler_params=params(0, 6),
    )(*[far_off(value) for value in (orders[None, :], jnp.asarray(table), plan, coeffs)])

    result = jax.ShapeDtypeStruct((share, rows), jnp.float32)
    copies = 1 + rows // IMAGES + share // IMAGES
    found = []
    for core, route in enumerate((routes[0] >> 8, routes[0] & 255)):
        rounds = [
            pl.pallas_call(
                functools.partial(round_kernel, core, offset),
                out_shape=(result, result),
                in_specs=[vmem, vmem, vmem, hbm, vmem],
                out_specs=(vmem, vmem),
                scratch_shapes=[
                    pltpu.VMEM((half, half), jnp.bfloat16),
                    pltpu.SMEM((3, LANES), jnp.int32),
                    pltpu.SemaphoreType.DMA,
                    pltpu.SemaphoreType.DMA,
                    pltpu.VMEM((rows, cols), jnp.bfloat16),
                    pltpu.VMEM((share, cols), jnp.bfloat16),
                    pltpu.VMEM((share, cols), jnp.bfloat16),
                    pltpu.VMEM((half // LANES, rows, 2 * LANES), jnp.bfloat16),
                    pltpu.VMEM((half // LANES, LANES, 2 * share), jnp.bfloat16),
                    pltpu.VMEM((rows * (2 * slots + 1), share), jnp.float32),
                    pltpu.VMEM((rows, share), jnp.float32),
                    pltpu.VMEM((rows, share), jnp.float32),
                    pltpu.VMEM((share, share), jnp.float32),
                    pltpu.VMEM((rows, share), jnp.float32),
                    pltpu.SemaphoreType.DMA((copies,)),
                    pltpu.SemaphoreType.DMA((copies,)),
                ],
                compiler_params=params(1 + core * chips + offset, 26),
            )
            for offset in range(chips)
        ]
        found += lax.switch(route, rounds, flips, marks, both, perm, angles)
    return pl.pallas_call(
        last_kernel,
        out_shape=jax.ShapeDtypeStruct((ROUNDS, share, rows), jnp.float32),
        in_specs=[vmem] * 4,
        out_specs=vmem,
        scratch_shapes=[pltpu.SemaphoreType.DMA] * 2,
        compiler_params=params(1 + 2 * chips, 8),
    )(*found)


def solution(mesh):
    n_blk, n_ang = mesh.shape["blk"], mesh.shape["ang"]
    body = per_device if n_blk <= 16 and n_ang == 2 else functools.partial(per_device_wide, routes(n_blk))
    return jax.shard_map(
        body,
        mesh=mesh,
        in_specs=(P("blk", None), P(), P()),
        out_specs=P(None, ("blk", "ang"), None),
        check_vma=False,
    )
```
